512 devices in a mesh: seq: 128 (over y, z, core), head: 4 (over x).
Axes of the slice: x: 4, y: 8, z: 8, core: 2. Of those that a mesh axis runs over, the one named last changes fastest.
Arguments:
- queries: bfloat16 [16384, 1536], P('seq', 'head'), may hold values from -400 to 400
- latent: bfloat16 [16384, 320], P(('seq', 'head')), may hold values from -6 to 6
- w_kv_up: bfloat16 [256, 2048], P(None, 'head'), may hold values from -0.375 to 0.375
Outputs:
- attended: bfloat16 [16384, 1024], P('seq', 'head')
The draws below stay inside these ranges and needn't reach their ends.
All inputs are finite; a program needn't handle non-finite values.
Results may differ from the reference program's by a relative error of at most 0.004.
Values may be sent and summed in bfloat16 or wider, within the bound.
No kernel may reach another device: no remote copies, remote signals or barrier semaphores. Data moves between devices by JAX's collectives and lax.ppermute only.
A program may use at most 64 MiB of HBM per device.

```python
import jax
import jax.numpy as jnp
from jax import lax

D_LATENT = 256
ROPE = 64
NOPE = 128
VDIM = 128
HEADS = 8
TOK_DEV = 128
SEQS = 1
LENGTH = 16384
TOKENS = 16384


def latent_field(key):
    sample = jax.random.normal(jax.random.fold_in(key, 11), (TOKENS, D_LATENT + ROPE), jnp.float32)
    return jnp.clip(sample, -6.0, 6.0)


def draw_latent(key, part):
    return latent_field(key).astype(jnp.bfloat16)


def draw_queries(key, part):
    sample = jax.random.normal(jax.random.fold_in(key, 23), (TOKENS, HEADS, NOPE + ROPE), jnp.float32)
    sample = 2.0 * jnp.clip(sample, -4.0, 4.0)
    return sample.reshape(TOKENS, HEADS * (NOPE + ROPE)).astype(jnp.bfloat16)


def shard_levels(stream_key, extent, cuts, smallest, top_value):
    def one(axis_at, parts):
        heights = jax.random.uniform(jax.random.fold_in(jax.random.fold_in(stream_key, 6), axis_at), (parts,), jnp.float32, smallest / len(cuts), top_value / len(cuts))
        return jnp.repeat(jnp.exp(heights), extent[axis_at] // parts).reshape((-1,) + (1,) * (len(extent) - axis_at - 1))

    loudness = one(*cuts[0])
    for cut in cuts[1:]:
        loudness = loudness * one(*cut)
    return loudness


def scatter_about(own_key, dims, deviation, most, cuts=(), kind=jnp.bfloat16):
    array = jax.random.normal(own_key, dims, jnp.float32) * deviation
    if len(cuts) > 0:
        array = shard_levels(own_key, dims, cuts, -0.22, 0.18) * array
    return jnp.clip(array, min=-most, max=most).astype(kind)


def setup_inputs(seed: int = 0) -> dict:
    keys = jax.random.split(jax.random.key(seed), 4)
    queries = draw_queries(jax.random.fold_in(keys[3], 71), 0)
    latent = draw_latent(jax.random.fold_in(keys[3], 71), 0)
    w_kv_up = scatter_about(keys[2], (D_LATENT, HEADS * (NOPE + VDIM)), D_LATENT ** -0.5, 0.375, ((1, 4),))
    return dict(queries=queries, latent=latent, w_kv_up=w_kv_up)


MASKED = -1e30


def reference(queries, latent, w_kv_up):
    head_width = NOPE + VDIM
    score_scale = (NOPE + ROPE) ** -0.5
    highest = lax.Precision.HIGHEST

    def one_sequence(seq_index):
        first_row = seq_index * LENGTH
        seq_latent = lax.dynamic_slice_in_dim(latent, first_row, LENGTH, 0)
        seq_queries = lax.dynamic_slice_in_dim(queries, first_row, LENGTH, 0)
        key_value = jnp.dot(seq_latent[:, :D_LATENT], w_kv_up, preferred_element_type=jnp.float32)
        key_value = key_value.reshape(LENGTH, HEADS, head_width)
        key_nope = key_value[:, :, :NOPE]
        values = key_value[:, :, NOPE:]
        key_rope = seq_latent[:, D_LATENT:].astype(jnp.float32)
        query_all = seq_queries.reshape(LENGTH, HEADS, NOPE + ROPE).astype(jnp.float32)
        blocks_out = []
        for block_index in range(LENGTH // TOK_DEV):
            low_row = block_index * TOK_DEV
            high_row = low_row + TOK_DEV
            query_block = query_all[low_row:high_row]
            scores = jnp.einsum('qhd,khd->hqk', query_block[:, :, :NOPE], key_nope[:high_row], precision=highest)
            scores = scores + jnp.einsum('qhd,kd->hqk', query_block[:, :, NOPE:], key_rope[:high_row], precision=highest)
            scores = scores * score_scale
            allowed = jnp.arange(high_row)[None, :] <= (low_row + jnp.arange(TOK_DEV))[:, None]
            scores = jnp.where(allowed[None], scores, MASKED)
            row_max = jnp.max(scores, axis=2, keepdims=True)
            weights = jnp.where(allowed[None], jnp.exp(scores - row_max), 0.0)
            totals = jnp.sum(weights, axis=2)
            rounded = lax.optimization_barrier(weights.astype(jnp.bfloat16)).astype(jnp.float32)
            summed = jnp.einsum('hqk,khd->hqd', rounded, values[:high_row], precision=highest)
            result = summed / totals[:, :, None]
            blocks_out.append(jnp.transpose(result, (1, 0, 2)).reshape(TOK_DEV, HEADS * VDIM))
        return jnp.concatenate(blocks_out, axis=0).astype(jnp.bfloat16)

    pieces = lax.map(one_sequence, jnp.arange(SEQS, dtype=jnp.int32))
    return pieces.reshape(TOKENS, HEADS * VDIM)
```

```python
import math

import jax
import jax.numpy as jnp
from jax import lax
from jax.experimental import pallas as pl
from jax.experimental.pallas import tpu as pltpu
from jax.sharding import Mesh
from jax.sharding import PartitionSpec as P

D_LATENT = 256
ROPE = 64
NOPE = 128
VDIM = 128
MASKED = -1e30
LOG2_SCALE = math.log2(math.e) * (NOPE + ROPE) ** -0.5


YS, ZS, CS, XS = 8, 8, 2, 4
GROUP = 128
KEYS = 32
UNIT = 2 * GROUP
CHUNK = ZS * KEYS
PACKED = KEYS * (D_LATENT + ROPE) // 128
QW_ROWS = 3 * GROUP + 4 * D_LATENT
OUT_ROWS = 2 * GROUP + 8
NT = (((1,), (1,)), ((), ()))
f32, bf16 = jnp.float32, jnp.bfloat16


def split(value):
    high = value.astype(bf16)
    return high, (value - high.astype(f32)).astype(bf16)


def prepare_queries(qw_ref, qcat_ref):
    lane = lax.broadcasted_iota(jnp.int32, (GROUP, 128), 1)
    for k in range(XS):
        rope = qw_ref[k, 2 * GROUP : 3 * GROUP].astype(f32) * LOG2_SCALE
        for h in range(2):
            nope = qw_ref[k, h * GROUP : (h + 1) * GROUP]
            start = 3 * GROUP + h * 2 * D_LATENT
            w_key = qw_ref[k, start : start + D_LATENT]
            side = lax.dot_general(nope, w_key, NT, preferred_element_type=f32) * LOG2_SCALE
            rows = pl.ds((2 * k + h) * GROUP, GROUP)
            high, low = split(side)
            qcat_ref[rows, 0:256] = high
            qcat_ref[rows, 256:512] = low
            turned = rope if h == 0 else pltpu.roll(rope, 64, 1)
            high, low = split(jnp.where(lane < ROPE, turned, 0.0))
            qcat_ref[rows, 512:640] = high
            qcat_ref[rows, 640:768] = low


def one_chunk(kv_ref, row, masks, qcat_ref, m_ref, l_ref, acc_ref):
    block = kv_ref[pl.ds(row * ZS, ZS)]
    latent = jnp.concatenate(
        [block[:, 0:KEYS].reshape(CHUNK, 128), block[:, KEYS : 2 * KEYS].reshape(CHUNK, 128)], axis=1
    )
    packed = block[:, 2 * KEYS :].astype(f32)
    other = pltpu.roll(packed.reshape(CHUNK // 2, 128), 64, 1).reshape(packed.shape)
    rope = jnp.concatenate([packed, other], axis=1).astype(bf16).reshape(CHUNK, 128)
    keys = jnp.concatenate([latent, latent, rope, rope], axis=1)
    for u in range(XS):
        rows = pl.ds(u * UNIT, UNIT)
        scores = lax.dot_general(qcat_ref[rows], keys, NT, preferred_element_type=f32)
        if masks is not None:
            scores = jnp.where(masks, scores, MASKED)
        m_old = m_ref[rows]
        m_new = jnp.maximum(m_old, jnp.max(scores, axis=1, keepdims=True))
        factor = jnp.exp2(m_old - m_new)
        weights = jnp.exp2(scores - jnp.concatenate([m_new, m_new], axis=1))
        if masks is not None:
            weights = jnp.where(masks, weights, 0.0)
        l_ref[rows] = l_ref[rows] * factor + jnp.sum(weights, axis=1, keepdims=True)
        update = jnp.dot(weights.astype(bf16), latent, preferred_element_type=f32)
        acc_ref[rows] = acc_ref[rows] * jnp.concatenate([factor, factor], axis=1) + update
        m_ref[rows] = m_new


def attend(kv_ref, from_other, qcat_ref, m_ref, l_ref, acc_ref):
    y, z, c, x = (lax.axis_index(a) for a in ("y", "z", "c", "x"))
    key_core = 1 - c if from_other else c
    row = lax.broadcasted_iota(jnp.int32, (UNIT, CHUNK), 0) % GROUP
    key = lax.broadcasted_iota(jnp.int32, (UNIT, CHUNK), 1)
    query_pos = (z * 2 + c) * GROUP + row
    key_pos = ((key // KEYS) * 2 + key_core) * GROUP + x * KEYS + key % KEYS
    refs = (qcat_ref, m_ref, l_ref, acc_ref)
    one_chunk(kv_ref, y, key_pos <= query_pos, *refs)
    lax.fori_loop(0, y, lambda i, _: one_chunk(kv_ref, i, None, *refs), None)


def first_kernel(qw_ref, kv_ref, qcat_ref, m_ref, l_ref, acc_ref):
    prepare_queries(qw_ref, qcat_ref)
    m_ref[...] = jnp.full(m_ref.shape, MASKED, f32)
    l_ref[...] = jnp.zeros(l_ref.shape, f32)
    acc_ref[...] = jnp.zeros(acc_ref.shape, f32)
    attend(kv_ref, False, qcat_ref, m_ref, l_ref, acc_ref)


def second_kernel(qw_ref, kv_ref, qcat_ref, m_in, l_in, acc_in, out_ref, m_ref, l_ref, acc_ref):
    m_ref[...] = m_in[...]
    l_ref[...] = l_in[...]
    acc_ref[...] = acc_in[...]
    attend(kv_ref, True, qcat_ref, m_ref, l_ref, acc_ref)
    x = lax.axis_index("x")
    eye = lax.broadcasted_iota(jnp.int32, (GROUP, 128), 0) == lax.broadcasted_iota(jnp.int32, (GROUP, 128), 1)
    for k in range(XS):
        owner = lax.rem(x + XS - k, XS)
        stats = []
        for h in range(2):
            rows = pl.ds((2 * k + h) * GROUP, GROUP)
            start = 3 * GROUP + h * 2 * D_LATENT + D_LATENT
            w_value = qw_ref[k, start : start + D_LATENT]
            high, low = split(acc_ref[rows])
            part = jnp.dot(high, w_value, preferred_element_type=f32)
            part = part + jnp.dot(low, w_value, preferred_element_type=f32)
            out_ref[owner, h * GROUP : (h + 1) * GROUP] = part
            for ref in (m_ref, l_ref):
                stats.append(jnp.sum(jnp.where(eye, ref[rows], 0.0), axis=0, keepdims=True))
        stats.append(jnp.zeros((4, 128), f32))
        out_ref[owner, 2 * GROUP :] = jnp.concatenate(stats, axis=0)


def combine_kernel(parts_ref, out_ref):
    eye = lax.broadcasted_iota(jnp.int32, (GROUP, 128), 0) == lax.broadcasted_iota(jnp.int32, (GROUP, 128), 1)
    for h in range(2):
        maxima = [parts_ref[k, 2 * GROUP + 2 * h : 2 * GROUP + 2 * h + 1] for k in range(XS)]
        totals = [parts_ref[k, 2 * GROUP + 2 * h + 1 : 2 * GROUP + 2 * h + 2] for k in range(XS)]
        top = jnp.maximum(jnp.maximum(maxima[0], maxima[1]), jnp.maximum(maxima[2], maxima[3]))
        factors = [jnp.exp2(m - top) for m in maxima]
        total = sum(f * t for f, t in zip(factors, totals))
        numerator = jnp.zeros((GROUP, 128), f32)
        for k in range(XS):
            column = jnp.sum(jnp.where(eye, factors[k] / total, 0.0), axis=1, keepdims=True)
            numerator = numerator + parts_ref[k, h * GROUP : (h + 1) * GROUP] * column
        out_ref[:, h * VDIM : (h + 1) * VDIM] = numerator.astype(bf16)


def call(kernel, out_shape, *args, scratch=()):
    return pl.pallas_call(
        kernel,
        out_shape=out_shape,
        in_specs=[pl.BlockSpec(memory_space=pltpu.VMEM)] * len(args),
        out_specs=jax.tree.map(lambda _: pl.BlockSpec(memory_space=pltpu.VMEM), out_shape),
        scratch_shapes=list(scratch),
    )(*args)


def pack_keys(latent):
    half = KEYS // 2
    rope = latent[:, D_LATENT:]
    return jnp.concatenate(
        [latent[:, :128], latent[:, 128:256], jnp.concatenate([rope[:half], rope[half:]], axis=1)], axis=0
    )


def pack_queries(queries, w_kv_up):
    wide = NOPE + ROPE
    return jnp.concatenate(
        [
            queries[:, :NOPE],
            queries[:, wide : wide + NOPE],
            jnp.concatenate([queries[:, NOPE:wide], queries[:, wide + NOPE :]], axis=1),
        ]
        + [w_kv_up[:, i * 128 : (i + 1) * 128] for i in range(4)],
        axis=0,
    )


def body(queries, latent, w_kv_up):
    packed = pack_keys(latent)
    with jax.named_scope("keys"):
        copies = jnp.broadcast_to(packed, (YS * ZS, PACKED, 128))
        mine = lax.all_to_all(copies, ("y", "z"), split_axis=0, concat_axis=0, tiled=True)
    with jax.named_scope("queries"):
        own = pack_queries(queries, w_kv_up)
        parts = [own] + [
            lax.ppermute(own, "x", [(i, (i + k) % XS) for i in range(XS)]) for k in range(1, XS)
        ]
        qw = jnp.stack(parts)
    with jax.named_scope("swap"):
        theirs = lax.ppermute(mine, "c", [(0, 1), (1, 0)])
    all_rows = XS * UNIT
    shapes = (
        jax.ShapeDtypeStruct((all_rows, 768), bf16),
        jax.ShapeDtypeStruct((all_rows, 128), f32),
        jax.ShapeDtypeStruct((all_rows, 128), f32),
        jax.ShapeDtypeStruct((all_rows, D_LATENT), f32),
    )
    qcat, m, l, acc = call(first_kernel, shapes, qw, mine)
    scratch = [pltpu.VMEM(s.shape, f32) for s in shapes[1:]]
    parts = call(
        second_kernel,
        jax.ShapeDtypeStruct((XS, OUT_ROWS, 128), f32),
        qw, theirs, qcat, m, l, acc,
        scratch=scratch,
    )
    parts = lax.all_to_all(parts, "x", split_axis=0, concat_axis=0, tiled=True)
    return call(combine_kernel, jax.ShapeDtypeStruct((GROUP, 2 * VDIM), bf16), parts)


def solution(mesh):
    mesh = Mesh(mesh.devices.reshape(YS, ZS, CS, XS), ("y", "z", "c", "x"))
    seq = ("y", "z", "c")
    in_specs = (P(seq, "x"), P((*seq, "x"), None), P(None, "x"))
    return jax.shard_map(body, mesh=mesh, in_specs=in_specs, out_specs=P(seq, "x"), check_vma=False)
```

```python
import math

import jax
import jax.numpy as jnp
from jax import lax
from jax.experimental import pallas as pl
from jax.experimental.pallas import tpu as pltpu
from jax.sharding import Mesh
from jax.sharding import PartitionSpec as P

D_LATENT = 256
ROPE = 64
NOPE = 128
VDIM = 128
MASKED = -1e30
LOG2_SCALE = math.log2(math.e) * (NOPE + ROPE) ** -0.5


YS, ZS, CS, XS = 8, 8, 2, 4
GROUP = 128
KEYS = 32
UNIT = 2 * GROUP
CHUNK = ZS * KEYS
PACKED = KEYS * (D_LATENT + ROPE) // 128
VMEM_LIMIT = 20 * 2**20
OUT_ROWS = 2 * VDIM + 16
NT = (((1,), (1,)), ((), ()))
f32, bf16 = jnp.float32, jnp.bfloat16


def split(value):
    high = value.astype(bf16)
    return high, (value - high.astype(f32)).astype(bf16)


def query_kernel(*refs):
    qcat_ref, values_ref = refs[XS:]
    for k in range(XS):
        qw_ref = refs[k]
        rope = qw_ref[2 * GROUP : 3 * GROUP].astype(f32).T * LOG2_SCALE
        for h in range(2):
            nope = qw_ref[h * GROUP : (h + 1) * GROUP]
            start = 3 * GROUP + h * 2 * D_LATENT
            w_key = qw_ref[start : start + D_LATENT]
            side = lax.dot_general(w_key, nope, NT, preferred_element_type=f32) * LOG2_SCALE
            values_ref[2 * k + h] = qw_ref[start + D_LATENT : start + 2 * D_LATENT].T
            cols = pl.ds((2 * k + h) * GROUP, GROUP)
            high, low = split(side)
            qcat_ref[0:256, cols] = high
            qcat_ref[256:512, cols] = low
            high, low = split(rope[h * ROPE : (h + 1) * ROPE])
            none = jnp.zeros((ROPE, GROUP), bf16)
            qcat_ref[512:768, cols] = jnp.concatenate([high, none, low, none], axis=0)


def one_chunk(kv_ref, row, masks, qcat_ref, m_ref, l_ref, acc_ref):
    block = kv_ref[pl.ds(row * ZS, ZS)]
    latent = jnp.concatenate(
        [block[:, 0:KEYS].reshape(CHUNK, 128), block[:, KEYS : 2 * KEYS].reshape(CHUNK, 128)], axis=1
    )
    packed = block[:, 2 * KEYS :].astype(f32)
    other = pltpu.roll(packed.reshape(CHUNK // 2, 128), 64, 1).reshape(packed.shape)
    rope = jnp.concatenate([packed, other], axis=1).astype(bf16).reshape(CHUNK, 128)
    keys = jnp.concatenate([latent, latent, rope, rope], axis=1)
    turned = latent.T
    units = [pl.ds(u * UNIT, UNIT) for u in range(XS)]
    scores = [jnp.dot(keys, qcat_ref[:, cols], preferred_element_type=f32) for cols in units]
    for u, cols in enumerate(units):
        s = scores[u]
        if masks is not None:
            s = jnp.where(masks, s, MASKED)
        m_old = m_ref[:, cols]
        m_new = jnp.maximum(m_old, jnp.max(s, axis=0, keepdims=True))
        factor = jnp.exp2(m_old - m_new)
        weights = jnp.exp2(s - m_new)
        if masks is not None:
            weights = jnp.where(masks, weights, 0.0)
        l_ref[:, cols] = l_ref[:, cols] * factor + jnp.sum(weights, axis=0, keepdims=True)
        m_ref[:, cols] = m_new
        update = jnp.dot(turned, weights.astype(bf16), preferred_element_type=f32)
        acc_ref[:, cols] = acc_ref[:, cols] * factor + update


def attend(kv_ref, from_other, qcat_ref, m_ref, l_ref, acc_ref):
    y, z, c, x = (lax.axis_index(a) for a in ("y", "z", "c", "x"))
    key_core = 1 - c if from_other else c
    key = lax.broadcasted_iota(jnp.int32, (CHUNK, UNIT), 0)
    row = lax.broadcasted_iota(jnp.int32, (CHUNK, UNIT), 1) % GROUP
    query_pos = (z * 2 + c) * GROUP + row
    key_pos = ((key // KEYS) * 2 + key_core) * GROUP + x * KEYS + key % KEYS
    refs = (qcat_ref, m_ref, l_ref, acc_ref)
    one_chunk(kv_ref, y, key_pos <= query_pos, *refs)
    lax.fori_loop(0, y, lambda i, _: one_chunk(kv_ref, i, None, *refs), None)


def first_kernel(kv_ref, qcat_ref, m_ref, l_ref, acc_ref):
    m_ref[...] = jnp.full(m_ref.shape, MASKED, f32)
    l_ref[...] = jnp.zeros(l_ref.shape, f32)
    acc_ref[...] = jnp.zeros(acc_ref.shape, f32)
    attend(kv_ref, False, qcat_ref, m_ref, l_ref, acc_ref)


def thirds(value):
    high, _ = split(value)
    middle, low = split(value - high.astype(f32))
    return [high, middle, low]


def second_kernel(values_ref, kv_ref, qcat_ref, m_in, l_in, acc_in, out_ref, m_ref, l_ref, acc_ref):
    m_ref[...] = m_in[...]
    l_ref[...] = l_in[...]
    acc_ref[...] = acc_in[...]
    attend(kv_ref, True, qcat_ref, m_ref, l_ref, acc_ref)
    x = lax.axis_index("x")
    for k in range(XS):
        owner = lax.rem(x + XS - k, XS)
        stats = []
        for h in range(2):
            cols = pl.ds((2 * k + h) * GROUP, GROUP)
            w_value = values_ref[2 * k + h]
            high, low = split(acc_ref[:, cols])
            part = jnp.dot(w_value, high, preferred_element_type=f32)
            part = part + jnp.dot(w_value, low, preferred_element_type=f32)
            out_ref[owner, h * VDIM : (h + 1) * VDIM] = part.astype(bf16)
            stats += thirds(m_ref[:, cols]) + thirds(l_ref[:, cols])
        stats.append(jnp.zeros((4, GROUP), bf16))
        out_ref[owner, 2 * VDIM :] = jnp.concatenate([t.astype(f32) for t in stats], axis=0).astype(bf16)


def combine_kernel(parts_ref, out_ref):
    stats = [parts_ref[k, 2 * VDIM :].astype(f32) for k in range(XS)]
    for h in range(2):

        def whole(k, at):
            row = 6 * h + 3 * at
            return stats[k][row : row + 1] + stats[k][row + 1 : row + 2] + stats[k][row + 2 : row + 3]

        maxima = [whole(k, 0) for k in range(XS)]
        top = jnp.maximum(jnp.maximum(maxima[0], maxima[1]), jnp.maximum(maxima[2], maxima[3]))
        factors = [jnp.exp2(m - top) for m in maxima]
        total = sum(f * whole(k, 1) for k, f in enumerate(factors))
        numerator = sum(
            parts_ref[k, h * VDIM : (h + 1) * VDIM].astype(f32) * (f / total) for k, f in enumerate(factors)
        )
        out_ref[:, h * VDIM : (h + 1) * VDIM] = numerator.T.astype(bf16)


def call(kernel, out_shape, *args, scratch=()):
    return pl.pallas_call(
        kernel,
        out_shape=out_shape,
        in_specs=[pl.BlockSpec(memory_space=pltpu.VMEM)] * len(args),
        out_specs=jax.tree.map(lambda _: pl.BlockSpec(memory_space=pltpu.VMEM), out_shape),
        scratch_shapes=list(scratch),
        compiler_params=pltpu.CompilerParams(vmem_limit_bytes=VMEM_LIMIT),
    )(*args)


def pack_keys(latent):
    half = KEYS // 2
    rope = latent[:, D_LATENT:]
    return jnp.concatenate(
        [latent[:, :128], latent[:, 128:256], jnp.concatenate([rope[:half], rope[half:]], axis=1)], axis=0
    )


def pack_queries(queries, w_kv_up):
    wide = NOPE + ROPE
    return jnp.concatenate(
        [
            queries[:, :NOPE],
            queries[:, wide : wide + NOPE],
            jnp.concatenate([queries[:, NOPE:wide], queries[:, wide + NOPE :]], axis=1),
        ]
        + [w_kv_up[:, i * 128 : (i + 1) * 128] for i in range(4)],
        axis=0,
    )


def steps(queries, latent, w_kv_up):
    packed = pack_keys(latent)
    copies = jnp.broadcast_to(packed, (YS * ZS, PACKED, 128))
    mine = lax.all_to_all(copies, ("y", "z"), split_axis=0, concat_axis=0, tiled=True)
    rows = XS * UNIT
    state = (
        jax.ShapeDtypeStruct((1, rows), f32),
        jax.ShapeDtypeStruct((1, rows), f32),
        jax.ShapeDtypeStruct((D_LATENT, rows), f32),
    )
    own = pack_queries(queries, w_kv_up)
    qws = [own] + [
        lax.ppermute(own, "x", [(i, (i + k) % XS) for i in range(XS)]) for k in range(1, XS)
    ]
    shapes = (
        jax.ShapeDtypeStruct((768, rows), bf16),
        jax.ShapeDtypeStruct((2 * XS, VDIM, D_LATENT), bf16),
    )
    qcat, values = call(query_kernel, shapes, *qws)
    theirs = lax.ppermute(mine, "c", [(0, 1), (1, 0)])
    m, l, acc = call(first_kernel, state, mine, qcat)
    scratch = [pltpu.VMEM(s.shape, f32) for s in state]
    parts = call(
        second_kernel,
        jax.ShapeDtypeStruct((XS, OUT_ROWS, 128), bf16),
        values, theirs, qcat, m, l, acc,
        scratch=scratch,
    )
    parts = lax.all_to_all(parts, "x", split_axis=0, concat_axis=0, tiled=True)
    return call(combine_kernel, jax.ShapeDtypeStruct((GROUP, 2 * VDIM), bf16), parts)


def solution(mesh):
    mesh = Mesh(mesh.devices.reshape(YS, ZS, CS, XS), ("y", "z", "c", "x"))
    seq = ("y", "z", "c")
    in_specs = (P(seq, "x"), P((*seq, "x"), None), P(None, "x"))
    return jax.shard_map(steps, mesh=mesh, in_specs=in_specs, out_specs=P(seq, "x"), check_vma=False)
```

```python
import functools
import math

import jax
import jax.numpy as jnp
from jax import lax
from jax.experimental import pallas as pl
from jax.experimental.pallas import tpu as pltpu
from jax.sharding import Mesh
from jax.sharding import PartitionSpec as P

D_LATENT = 256
ROPE = 64
NOPE = 128
VDIM = 128
MASKED = -1e30
LOWEST = -0.5e30
LOG2_SCALE = math.log2(math.e) * (NOPE + ROPE) ** -0.5


YS, ZH, ZL, CS, XS = 8, 4, 2, 2, 4
GROUP = 128
KEYS = 32
UNIT = 2 * GROUP
SPAN = 4
CHUNK = SPAN * ZH * KEYS
PACKED = KEYS * (D_LATENT + ROPE) // 128
VMEM_LIMIT = 20 * 2**20
OUT_ROWS = 2 * VDIM + 16
NT = (((1,), (1,)), ((), ()))
f32, bf16 = jnp.float32, jnp.bfloat16


def split(value):
    high = value.astype(bf16)
    return high, (value - high.astype(f32)).astype(bf16)


def query_kernel(*refs):
    qcat_ref, values_ref = refs[XS:]
    for k in range(XS):
        qw_ref = refs[k]
        rope = qw_ref[2 * GROUP : 3 * GROUP].astype(f32).T * LOG2_SCALE
        for h in range(2):
            nope = qw_ref[h * GROUP : (h + 1) * GROUP]
            start = 3 * GROUP + h * 2 * D_LATENT
            w_key = qw_ref[start : start + D_LATENT]
            side = lax.dot_general(w_key, nope, NT, preferred_element_type=f32) * LOG2_SCALE
            values_ref[2 * k + h] = qw_ref[start + D_LATENT : start + 2 * D_LATENT].T
            cols = pl.ds((2 * k + h) * GROUP, GROUP)
            high, low = split(side)
            qcat_ref[0:256, cols] = high
            qcat_ref[256:512, cols] = low
            high, low = split(rope[h * ROPE : (h + 1) * ROPE])
            none = jnp.zeros((ROPE, GROUP), bf16)
            qcat_ref[512:768, cols] = jnp.concatenate([high, none, low, none], axis=0)


def one_chunk(kv_ref, index, allowed, qcat_ref, m_ref, l_ref, acc_ref):
    block = kv_ref[pl.ds(index * SPAN * ZH, SPAN * ZH)]
    latent = jnp.concatenate(
        [block[:, 0:KEYS].reshape(CHUNK, 128), block[:, KEYS : 2 * KEYS].reshape(CHUNK, 128)], axis=1
    )
    packed = block[:, 2 * KEYS :].astype(f32)
    other = pltpu.roll(packed.reshape(CHUNK // 2, 128), 64, 1).reshape(packed.shape)
    rope = jnp.concatenate([packed, other], axis=1).astype(bf16).reshape(CHUNK, 128)
    keys = jnp.concatenate([latent, latent, rope, rope], axis=1)
    turned = latent.T
    units = [pl.ds(u * UNIT, UNIT) for u in range(XS)]
    scores = [jnp.dot(keys, qcat_ref[:, cols], preferred_element_type=f32) for cols in units]
    for s, cols in zip(scores, units):
        if allowed is not None:
            s = jnp.where(allowed, s, MASKED)
        m_old = m_ref[:, cols]
        m_new = jnp.maximum(m_old, jnp.max(s, axis=0, keepdims=True))
        factor = jnp.exp2(m_old - m_new)
        weights = jnp.exp2(s - m_new)
        l_ref[:, cols] = l_ref[:, cols] * factor + jnp.sum(weights, axis=0, keepdims=True)
        m_ref[:, cols] = m_new
        update = jnp.dot(turned, weights.astype(bf16), preferred_element_type=f32)
        acc_ref[:, cols] = acc_ref[:, cols] * factor + update


def attend(kv_ref, same_parity, same_core, qcat_ref, m_ref, l_ref, acc_ref):
    y, zh, zl, c, x = (lax.axis_index(a) for a in ("y", "zh", "zl", "c", "x"))
    key_zl = zl if same_parity else 1 - zl
    key_c = c if same_core else 1 - c
    last = y // SPAN
    key = lax.broadcasted_iota(jnp.int32, (CHUNK, UNIT), 0)
    row = lax.broadcasted_iota(jnp.int32, (CHUNK, UNIT), 1) % GROUP
    query_pos = (((y * ZH + zh) * ZL + zl) * CS + c) * GROUP + row
    key_group = ((last * SPAN * ZH + key // KEYS) * ZL + key_zl) * CS + key_c
    key_pos = key_group * GROUP + x * KEYS + key % KEYS
    refs = (qcat_ref, m_ref, l_ref, acc_ref)
    one_chunk(kv_ref, last, key_pos <= query_pos, *refs)
    lax.fori_loop(0, last, lambda i, _: one_chunk(kv_ref, i, None, *refs), None)


def attend_first(kv_ref, qcat_ref, m_ref, l_ref, acc_ref):
    m_ref[...] = jnp.full(m_ref.shape, LOWEST, f32)
    l_ref[...] = jnp.zeros(l_ref.shape, f32)
    acc_ref[...] = jnp.zeros(acc_ref.shape, f32)
    attend(kv_ref, True, True, qcat_ref, m_ref, l_ref, acc_ref)


def attend_more(same_parity, same_core, kv_ref, qcat_ref, m_in, l_in, acc_in, m_ref, l_ref, acc_ref):
    m_ref[...] = m_in[...]
    l_ref[...] = l_in[...]
    acc_ref[...] = acc_in[...]
    attend(kv_ref, same_parity, same_core, qcat_ref, m_ref, l_ref, acc_ref)


def thirds(value):
    high, _ = split(value)
    middle, low = split(value - high.astype(f32))
    return [high, middle, low]


def attend_last(values_ref, kv_ref, qcat_ref, m_in, l_in, acc_in, out_ref, m_ref, l_ref, acc_ref):
    attend_more(False, False, kv_ref, qcat_ref, m_in, l_in, acc_in, m_ref, l_ref, acc_ref)
    x = lax.axis_index("x")
    for k in range(XS):
        owner = lax.rem(x + XS - k, XS)
        stats = []
        for h in range(2):
            cols = pl.ds((2 * k + h) * GROUP, GROUP)
            w_value = values_ref[2 * k + h]
            high, low = split(acc_ref[:, cols])
            part = jnp.dot(w_value, high, preferred_element_type=f32)
            part = part + jnp.dot(w_value, low, preferred_element_type=f32)
            out_ref[owner, h * VDIM : (h + 1) * VDIM] = part.astype(bf16)
            stats += thirds(m_ref[:, cols]) + thirds(l_ref[:, cols])
        stats.append(jnp.zeros((4, GROUP), bf16))
        out_ref[owner, 2 * VDIM :] = jnp.concatenate([t.astype(f32) for t in stats], axis=0).astype(bf16)


def combine_kernel(parts_ref, out_ref):
    stats = [parts_ref[k, 2 * VDIM :].astype(f32) for k in range(XS)]
    for h in range(2):

        def whole(k, at):
            row = 6 * h + 3 * at
            return stats[k][row : row + 1] + stats[k][row + 1 : row + 2] + stats[k][row + 2 : row + 3]

        maxima = [whole(k, 0) for k in range(XS)]
        top = jnp.maximum(jnp.maximum(maxima[0], maxima[1]), jnp.maximum(maxima[2], maxima[3]))
        factors = [jnp.exp2(m - top) for m in maxima]
        total = sum(f * whole(k, 1) for k, f in enumerate(factors))
        numerator = sum(
            parts_ref[k, h * VDIM : (h + 1) * VDIM].astype(f32) * (f / total) for k, f in enumerate(factors)
        )
        out_ref[:, h * VDIM : (h + 1) * VDIM] = numerator.T.astype(bf16)


def call(kernel, out_shape, *args, scratch=()):
    return pl.pallas_call(
        kernel,
        out_shape=out_shape,
        in_specs=[pl.BlockSpec(memory_space=pltpu.VMEM)] * len(args),
        out_specs=jax.tree.map(lambda _: pl.BlockSpec(memory_space=pltpu.VMEM), out_shape),
        scratch_shapes=list(scratch),
        compiler_params=pltpu.CompilerParams(vmem_limit_bytes=VMEM_LIMIT),
    )(*args)


def pack_kernel(latent_ref, out_ref):
    half = KEYS // 2
    rows = latent_ref[...].astype(f32)
    rope = jnp.concatenate([rows[:half, D_LATENT:], rows[half:, D_LATENT:]], axis=1)
    packed = jnp.concatenate([rows[:, :128], rows[:, 128:256], rope], axis=0).astype(bf16)
    for i in range(YS * ZH):
        out_ref[i] = packed


def pack_queries(queries, w_kv_up):
    wide = NOPE + ROPE
    return jnp.concatenate(
        [
            queries[:, :NOPE],
            queries[:, wide : wide + NOPE],
            jnp.concatenate([queries[:, NOPE:wide], queries[:, wide + NOPE :]], axis=1),
        ]
        + [w_kv_up[:, i * 128 : (i + 1) * 128] for i in range(4)],
        axis=0,
    )


def steps(queries, latent, w_kv_up):
    copies = call(pack_kernel, jax.ShapeDtypeStruct((YS * ZH, PACKED, 128), bf16), latent)
    near = lax.all_to_all(copies, ("y", "zh"), split_axis=0, concat_axis=0, tiled=True)
    rows = XS * UNIT
    state = (
        jax.ShapeDtypeStruct((1, rows), f32),
        jax.ShapeDtypeStruct((1, rows), f32),
        jax.ShapeDtypeStruct((D_LATENT, rows), f32),
    )
    own = pack_queries(queries, w_kv_up)
    qws = [own] + [
        lax.ppermute(own, "x", [(i, (i + k) % XS) for i in range(XS)]) for k in range(1, XS)
    ]
    shapes = (
        jax.ShapeDtypeStruct((768, rows), bf16),
        jax.ShapeDtypeStruct((2 * XS, VDIM, D_LATENT), bf16),
    )
    qcat, values = call(query_kernel, shapes, *qws)
    zs, middle = ZH * ZL, YS * ZH // 2
    low = lax.ppermute(near[:middle], ("zh", "zl"), [(i, (i + 1) % zs) for i in range(zs)])
    high = lax.ppermute(near[middle:], ("zh", "zl"), [(i, (i - 1) % zs) for i in range(zs)])
    swap = [(0, 1), (1, 0)]
    near_other = lax.ppermute(near, "c", swap)
    m, l, acc = call(attend_first, state, near, qcat)
    m, l, acc = call(functools.partial(attend_more, True, False), state, near_other, qcat, m, l, acc)
    far = jnp.concatenate([low, high])
    far_other = lax.ppermute(far, "c", swap)
    m, l, acc = call(functools.partial(attend_more, False, True), state, far, qcat, m, l, acc)
    parts = call(
        attend_last,
        jax.ShapeDtypeStruct((XS, OUT_ROWS, 128), bf16),
        values, far_other, qcat, m, l, acc,
        scratch=[pltpu.VMEM(s.shape, f32) for s in state],
    )
    parts = lax.all_to_all(parts, "x", split_axis=0, concat_axis=0, tiled=True)
    return call(combine_kernel, jax.ShapeDtypeStruct((GROUP, 2 * VDIM), bf16), parts)


def solution(mesh):
    mesh = Mesh(mesh.devices.reshape(YS, ZH, ZL, CS, XS), ("y", "zh", "zl", "c", "x"))
    seq = ("y", "zh", "zl", "c")
    in_specs = (P(seq, "x"), P((*seq, "x"), None), P(None, "x"))
    return jax.shard_map(steps, mesh=mesh, in_specs=in_specs, out_specs=P(seq, "x"), check_vma=False)
```

```python
import functools
import math

import jax
import jax.numpy as jnp
from jax import lax
from jax.experimental import pallas as pl
from jax.experimental.pallas import tpu as pltpu
from jax.sharding import Mesh
from jax.sharding import PartitionSpec as P

D_LATENT = 256
ROPE = 64
NOPE = 128
VDIM = 128
MASKED = -1e30
LOWEST = -0.5e30
LOG2_SCALE = math.log2(math.e) * (NOPE + ROPE) ** -0.5


YS, ZH, ZL, CS, XS = 8, 4, 2, 2, 4
GROUP = 128
KEYS = 32
UNIT = 2 * GROUP
HALF = YS * ZH // 2
PACKED = KEYS * (D_LATENT + ROPE) // 128
VMEM_LIMIT = 20 * 2**20
OUT_ROWS = 2 * VDIM + 16
NT = (((1,), (1,)), ((), ()))
f32, bf16 = jnp.float32, jnp.bfloat16


def split(value):
    high = value.astype(bf16)
    return high, (value - high.astype(f32)).astype(bf16)


def query_kernel(*refs):
    qcat_ref, values_ref = refs[XS:]
    for k in range(XS):
        qw_ref = refs[k]
        rope = qw_ref[2 * GROUP : 3 * GROUP].astype(f32).T * LOG2_SCALE
        for h in range(2):
            nope = qw_ref[h * GROUP : (h + 1) * GROUP]
            start = 3 * GROUP + h * 2 * D_LATENT
            w_key = qw_ref[start : start + D_LATENT]
            side = lax.dot_general(w_key, nope, NT, preferred_element_type=f32) * LOG2_SCALE
            values_ref[2 * k + h] = qw_ref[start + D_LATENT : start + 2 * D_LATENT].T
            cols = pl.ds((2 * k + h) * GROUP, GROUP)
            high, low = split(side)
            qcat_ref[0:256, cols] = high
            qcat_ref[256:512, cols] = low
            high, low = split(rope[h * ROPE : (h + 1) * ROPE])
            none = jnp.zeros((ROPE, GROUP), bf16)
            qcat_ref[512:768, cols] = jnp.concatenate([high, none, low, none], axis=0)


def attend_groups(groups, kv_ref, key_zl, key_c, qcat_ref, old, new):
    y, zh, zl, c, x = (lax.axis_index(a) for a in ("y", "zh", "zl", "c", "x"))
    count, free = groups * KEYS, (groups - HALF) * KEYS
    block = kv_ref[0:groups]
    latent = jnp.concatenate(
        [block[:, 0:KEYS].reshape(count, 128), block[:, KEYS : 2 * KEYS].reshape(count, 128)], axis=1
    )
    packed = block[:, 2 * KEYS :].astype(f32)
    other = pltpu.roll(packed.reshape(count // 2, 128), 64, 1).reshape(packed.shape)
    rope = jnp.concatenate([packed, other], axis=1).astype(bf16).reshape(count, 128)
    keys = jnp.concatenate([latent, latent, rope, rope], axis=1)
    turned = latent.T
    key = free + lax.broadcasted_iota(jnp.int32, (count - free, UNIT), 0)
    row = lax.broadcasted_iota(jnp.int32, (count - free, UNIT), 1) % GROUP
    query_pos = (((y * ZH + zh) * ZL + zl) * CS + c) * GROUP + row
    key_pos = (((key // KEYS) * ZL + key_zl) * CS + key_c) * GROUP + x * KEYS + key % KEYS
    allowed = key_pos <= query_pos
    m_ref, l_ref, acc_ref = new
    units = [pl.ds(u * UNIT, UNIT) for u in range(XS)]
    scores = [jnp.dot(keys, qcat_ref[:, cols], preferred_element_type=f32) for cols in units]
    for s, cols in zip(scores, units):
        masked = jnp.where(allowed, s[free:], MASKED)
        s = jnp.concatenate([s[:free], masked], axis=0) if free else masked
        top = jnp.max(s, axis=0, keepdims=True)
        top = jnp.maximum(top, LOWEST if old is None else old[0][:, cols])
        weights = jnp.exp2(s - top)
        total = jnp.sum(weights, axis=0, keepdims=True)
        update = jnp.dot(turned, weights.astype(bf16), preferred_element_type=f32)
        if old is not None:
            factor = jnp.exp2(old[0][:, cols] - top)
            total = total + old[1][:, cols] * factor
            update = update + old[2][:, cols] * factor
        m_ref[:, cols], l_ref[:, cols], acc_ref[:, cols] = top, total, update


def attend(same_parity, same_core, kv_ref, qcat_ref, old, new):
    zl, c = lax.axis_index("zl"), lax.axis_index("c")
    key_zl = zl if same_parity else 1 - zl
    key_c = c if same_core else 1 - c
    upper = lax.axis_index("y") >= YS // 2

    @pl.when(upper)
    def _():
        attend_groups(2 * HALF, kv_ref, key_zl, key_c, qcat_ref, old, new)

    @pl.when(jnp.logical_not(upper))
    def _():
        attend_groups(HALF, kv_ref, key_zl, key_c, qcat_ref, old, new)


def attend_first(kv_ref, qcat_ref, m_ref, l_ref, acc_ref):
    attend(True, True, kv_ref, qcat_ref, None, (m_ref, l_ref, acc_ref))


def attend_more(same_parity, same_core, kv_ref, qcat_ref, m_in, l_in, acc_in, m_ref, l_ref, acc_ref):
    attend(same_parity, same_core, kv_ref, qcat_ref, (m_in, l_in, acc_in), (m_ref, l_ref, acc_ref))


def thirds(value):
    high, _ = split(value)
    middle, low = split(value - high.astype(f32))
    return [high, middle, low]


def attend_last(values_ref, kv_ref, qcat_ref, m_in, l_in, acc_in, out_ref, m_ref, l_ref, acc_ref):
    attend_more(False, False, kv_ref, qcat_ref, m_in, l_in, acc_in, m_ref, l_ref, acc_ref)
    x = lax.axis_index("x")
    for k in range(XS):
        owner = lax.rem(x + XS - k, XS)
        stats = []
        for h in range(2):
            cols = pl.ds((2 * k + h) * GROUP, GROUP)
            w_value = values_ref[2 * k + h]
            high, low = split(acc_ref[:, cols])
            part = jnp.dot(w_value, high, preferred_element_type=f32)
            part = part + jnp.dot(w_value, low, preferred_element_type=f32)
            out_ref[owner, h * VDIM : (h + 1) * VDIM] = part.astype(bf16)
            stats += thirds(m_ref[:, cols]) + thirds(l_ref[:, cols])
        stats.append(jnp.zeros((4, GROUP), bf16))
        out_ref[owner, 2 * VDIM :] = jnp.concatenate([t.astype(f32) for t in stats], axis=0).astype(bf16)


def combine_kernel(parts_ref, out_ref):
    stats = [parts_ref[k, 2 * VDIM :].astype(f32) for k in range(XS)]
    for h in range(2):

        def whole(k, at):
            row = 6 * h + 3 * at
            return stats[k][row : row + 1] + stats[k][row + 1 : row + 2] + stats[k][row + 2 : row + 3]

        maxima = [whole(k, 0) for k in range(XS)]
        top = jnp.maximum(jnp.maximum(maxima[0], maxima[1]), jnp.maximum(maxima[2], maxima[3]))
        factors = [jnp.exp2(m - top) for m in maxima]
        total = sum(f * whole(k, 1) for k, f in enumerate(factors))
        numerator = sum(
            parts_ref[k, h * VDIM : (h + 1) * VDIM].astype(f32) * (f / total) for k, f in enumerate(factors)
        )
        out_ref[:, h * VDIM : (h + 1) * VDIM] = numerator.T.astype(bf16)


def call(kernel, out_shape, *args, scratch=()):
    return pl.pallas_call(
        kernel,
        out_shape=out_shape,
        in_specs=[pl.BlockSpec(memory_space=pltpu.VMEM)] * len(args),
        out_specs=jax.tree.map(lambda _: pl.BlockSpec(memory_space=pltpu.VMEM), out_shape),
        scratch_shapes=list(scratch),
        compiler_params=pltpu.CompilerParams(vmem_limit_bytes=VMEM_LIMIT),
    )(*args)


def pack_kernel(latent_ref, out_ref):
    half = KEYS // 2
    rows = latent_ref[...].astype(f32)
    rope = jnp.concatenate([rows[:half, D_LATENT:], rows[half:, D_LATENT:]], axis=1)
    packed = jnp.concatenate([rows[:, :128], rows[:, 128:256], rope], axis=0).astype(bf16)
    for i in range(YS * ZH):
        out_ref[i] = packed


def pack_queries(queries, w_kv_up):
    wide = NOPE + ROPE
    return jnp.concatenate(
        [
            queries[:, :NOPE],
            queries[:, wide : wide + NOPE],
            jnp.concatenate([queries[:, NOPE:wide], queries[:, wide + NOPE :]], axis=1),
        ]
        + [w_kv_up[:, i * 128 : (i + 1) * 128] for i in range(4)],
        axis=0,
    )


def steps(queries, latent, w_kv_up):
    copies = call(pack_kernel, jax.ShapeDtypeStruct((YS * ZH, PACKED, 128), bf16), latent)
    near = lax.all_to_all(copies, ("y", "zh"), split_axis=0, concat_axis=0, tiled=True)
    rows = XS * UNIT
    state = (
        jax.ShapeDtypeStruct((1, rows), f32),
        jax.ShapeDtypeStruct((1, rows), f32),
        jax.ShapeDtypeStruct((D_LATENT, rows), f32),
    )
    own = pack_queries(queries, w_kv_up)
    qws = [own] + [
        lax.ppermute(own, "x", [(i, (i + k) % XS) for i in range(XS)]) for k in range(1, XS)
    ]
    shapes = (
        jax.ShapeDtypeStruct((768, rows), bf16),
        jax.ShapeDtypeStruct((2 * XS, VDIM, D_LATENT), bf16),
    )
    qcat, values = call(query_kernel, shapes, *qws)
    zs, middle = ZH * ZL, YS * ZH // 2
    low = lax.ppermute(near[:middle], ("zh", "zl"), [(i, (i + 1) % zs) for i in range(zs)])
    high = lax.ppermute(near[middle:], ("zh", "zl"), [(i, (i - 1) % zs) for i in range(zs)])
    swap = [(0, 1), (1, 0)]
    near_other = lax.ppermute(near, "c", swap)
    m, l, acc = call(attend_first, state, near, qcat)
    m, l, acc = call(functools.partial(attend_more, True, False), state, near_other, qcat, m, l, acc)
    far = jnp.concatenate([low, high])
    far_other = lax.ppermute(far, "c", swap)
    m, l, acc = call(functools.partial(attend_more, False, True), state, far, qcat, m, l, acc)
    parts = call(
        attend_last,
        jax.ShapeDtypeStruct((XS, OUT_ROWS, 128), bf16),
        values, far_other, qcat, m, l, acc,
        scratch=[pltpu.VMEM(s.shape, f32) for s in state],
    )
    parts = lax.all_to_all(parts, "x", split_axis=0, concat_axis=0, tiled=True)
    return call(combine_kernel, jax.ShapeDtypeStruct((GROUP, 2 * VDIM), bf16), parts)


def solution(mesh):
    mesh = Mesh(mesh.devices.reshape(YS, ZH, ZL, CS, XS), ("y", "zh", "zl", "c", "x"))
    seq = ("y", "zh", "zl", "c")
    in_specs = (P(seq, "x"), P((*seq, "x"), None), P(None, "x"))
    return jax.shard_map(steps, mesh=mesh, in_specs=in_specs, out_specs=P(seq, "x"), check_vma=False)
```

```python
import functools
import math

import jax
import jax.numpy as jnp
from jax import lax
from jax.experimental import pallas as pl
from jax.experimental.pallas import tpu as pltpu
from jax.sharding import Mesh
from jax.sharding import PartitionSpec as P

D_LATENT = 256
ROPE = 64
NOPE = 128
VDIM = 128
MASKED = -1e30
LOWEST = -0.5e30
LOG2_SCALE = math.log2(math.e) * (NOPE + ROPE) ** -0.5


YS, ZH, ZL, CS, XS = 8, 4, 2, 2, 4
GROUP = 128
KEYS = 32
UNIT = 2 * GROUP
HALF = YS * ZH // 2
PACKED = KEYS * (D_LATENT + ROPE) // 128
VMEM_LIMIT = 20 * 2**20
OUT_ROWS = 2 * VDIM + 16
NT = (((1,), (1,)), ((), ()))
f32, bf16 = jnp.float32, jnp.bfloat16


def split(value):
    high = value.astype(bf16)
    return high, (value - high.astype(f32)).astype(bf16)


def query_kernel(*refs):
    qcat_ref, values_ref = refs[XS:]
    for k in range(XS):
        qw_ref = refs[k]
        rope = qw_ref[2 * GROUP : 3 * GROUP].astype(f32).T * LOG2_SCALE
        for h in range(2):
            nope = qw_ref[h * GROUP : (h + 1) * GROUP]
            start = 3 * GROUP + h * 2 * D_LATENT
            w_key = qw_ref[start : start + D_LATENT]
            side = lax.dot_general(w_key, nope, NT, preferred_element_type=f32) * LOG2_SCALE
            values_ref[2 * k + h] = qw_ref[start + D_LATENT : start + 2 * D_LATENT].T
            cols = pl.ds((2 * k + h) * GROUP, GROUP)
            high, low = split(side)
            qcat_ref[0:256, cols] = high
            qcat_ref[256:512, cols] = low
            high, low = split(rope[h * ROPE : (h + 1) * ROPE])
            none = jnp.zeros((ROPE, GROUP), bf16)
            qcat_ref[512:768, cols] = jnp.concatenate([high, none, low, none], axis=0)


def attend_groups(groups, kv_ref, key_zl, key_c, qcat_ref, old, new):
    y, zh, zl, c, x = (lax.axis_index(a) for a in ("y", "zh", "zl", "c", "x"))
    count, free = groups * KEYS, (groups - HALF) * KEYS
    block = kv_ref[0:groups]
    latent = jnp.concatenate(
        [block[:, 0:KEYS].reshape(count, 128), block[:, KEYS : 2 * KEYS].reshape(count, 128)], axis=1
    )
    packed = block[:, 2 * KEYS :].astype(f32)
    other = pltpu.roll(packed.reshape(count // 2, 128), 64, 1).reshape(packed.shape)
    rope = jnp.concatenate([packed, other], axis=1).astype(bf16).reshape(count, 128)
    keys = jnp.concatenate([latent, latent, rope, rope], axis=1)
    turned = latent.T
    key = free + lax.broadcasted_iota(jnp.int32, (count - free, UNIT), 0)
    row = lax.broadcasted_iota(jnp.int32, (count - free, UNIT), 1) % GROUP
    query_pos = (((y * ZH + zh) * ZL + zl) * CS + c) * GROUP + row
    key_pos = (((key // KEYS) * ZL + key_zl) * CS + key_c) * GROUP + x * KEYS + key % KEYS
    allowed = key_pos <= query_pos
    m_ref, l_ref, acc_ref = new
    units = [pl.ds(u * UNIT, UNIT) for u in range(XS)]
    scores = [jnp.dot(keys, qcat_ref[:, cols], preferred_element_type=f32) for cols in units]
    for s, cols in zip(scores, units):
        masked = jnp.where(allowed, s[free:], MASKED)
        s = jnp.concatenate([s[:free], masked], axis=0) if free else masked
        top = jnp.max(s, axis=0, keepdims=True)
        top = jnp.maximum(top, LOWEST if old is None else old[0][:, cols])
        weights = jnp.exp2(s - top)
        total = jnp.sum(weights, axis=0, keepdims=True)
        update = jnp.dot(turned, weights.astype(bf16), preferred_element_type=f32)
        if old is not None:
            factor = jnp.exp2(old[0][:, cols] - top)
            total = total + old[1][:, cols] * factor
            update = update + old[2][:, cols] * factor
        m_ref[:, cols], l_ref[:, cols], acc_ref[:, cols] = top, total, update


def attend(same_parity, same_core, kv_ref, qcat_ref, old, new):
    zl, c = lax.axis_index("zl"), lax.axis_index("c")
    key_zl = zl if same_parity else 1 - zl
    key_c = c if same_core else 1 - c
    upper = lax.axis_index("y") >= YS // 2

    @pl.when(upper)
    def _():
        attend_groups(2 * HALF, kv_ref, key_zl, key_c, qcat_ref, old, new)

    @pl.when(jnp.logical_not(upper))
    def _():
        attend_groups(HALF, kv_ref, key_zl, key_c, qcat_ref, old, new)


def attend_first(kv_ref, qcat_ref, m_ref, l_ref, acc_ref):
    attend(True, True, kv_ref, qcat_ref, None, (m_ref, l_ref, acc_ref))


def attend_more(same_parity, same_core, kv_ref, qcat_ref, m_in, l_in, acc_in, m_ref, l_ref, acc_ref):
    attend(same_parity, same_core, kv_ref, qcat_ref, (m_in, l_in, acc_in), (m_ref, l_ref, acc_ref))


def thirds(value):
    high, _ = split(value)
    middle, low = split(value - high.astype(f32))
    return [high, middle, low]


def attend_last(values_ref, kv_ref, qcat_ref, m_in, l_in, acc_in, out_ref, m_ref, l_ref, acc_ref):
    attend_more(False, False, kv_ref, qcat_ref, m_in, l_in, acc_in, m_ref, l_ref, acc_ref)
    x = lax.axis_index("x")
    for k in range(XS):
        owner = lax.rem(x + XS - k, XS)
        stats = []
        for h in range(2):
            cols = pl.ds((2 * k + h) * GROUP, GROUP)
            w_value = values_ref[2 * k + h]
            high, low = split(acc_ref[:, cols])
            part = jnp.dot(w_value, high, preferred_element_type=f32)
            part = part + jnp.dot(w_value, low, preferred_element_type=f32)
            out_ref[owner, h * VDIM : (h + 1) * VDIM] = part.astype(bf16)
            stats += thirds(m_ref[:, cols]) + thirds(l_ref[:, cols])
        stats.append(jnp.zeros((4, GROUP), bf16))
        out_ref[owner, 2 * VDIM :] = jnp.concatenate([t.astype(f32) for t in stats], axis=0).astype(bf16)


def combine_kernel(parts_ref, out_ref):
    stats = [parts_ref[k, 2 * VDIM :].astype(f32) for k in range(XS)]
    for h in range(2):

        def whole(k, at):
            row = 6 * h + 3 * at
            return stats[k][row : row + 1] + stats[k][row + 1 : row + 2] + stats[k][row + 2 : row + 3]

        maxima = [whole(k, 0) for k in range(XS)]
        top = jnp.maximum(jnp.maximum(maxima[0], maxima[1]), jnp.maximum(maxima[2], maxima[3]))
        factors = [jnp.exp2(m - top) for m in maxima]
        total = sum(f * whole(k, 1) for k, f in enumerate(factors))
        numerator = sum(
            parts_ref[k, h * VDIM : (h + 1) * VDIM].astype(f32) * (f / total) for k, f in enumerate(factors)
        )
        out_ref[:, h * VDIM : (h + 1) * VDIM] = numerator.T.astype(bf16)


def call(kernel, out_shape, *args, scratch=()):
    return pl.pallas_call(
        kernel,
        out_shape=out_shape,
        in_specs=[pl.BlockSpec(memory_space=pltpu.VMEM)] * len(args),
        out_specs=jax.tree.map(lambda _: pl.BlockSpec(memory_space=pltpu.VMEM), out_shape),
        scratch_shapes=list(scratch),
        compiler_params=pltpu.CompilerParams(vmem_limit_bytes=VMEM_LIMIT),
    )(*args)


def pack_kernel(latent_ref, out_ref):
    half = KEYS // 2
    rows = latent_ref[...].astype(f32)
    rope = jnp.concatenate([rows[:half, D_LATENT:], rows[half:, D_LATENT:]], axis=1)
    packed = jnp.concatenate([rows[:, :128], rows[:, 128:256], rope], axis=0).astype(bf16)
    for i in range(YS * ZH):
        out_ref[i] = packed


def pack_queries(queries, w_kv_up):
    wide = NOPE + ROPE
    return jnp.concatenate(
        [
            queries[:, :NOPE],
            queries[:, wide : wide + NOPE],
            jnp.concatenate([queries[:, NOPE:wide], queries[:, wide + NOPE :]], axis=1),
        ]
        + [w_kv_up[:, i * 128 : (i + 1) * 128] for i in range(4)],
        axis=0,
    )


def steps(queries, latent, w_kv_up):
    copies = call(pack_kernel, jax.ShapeDtypeStruct((YS * ZH, PACKED, 128), bf16), latent)
    near = lax.all_to_all(copies, ("y", "zh"), split_axis=0, concat_axis=0, tiled=True)
    rows = XS * UNIT
    state = (
        jax.ShapeDtypeStruct((1, rows), f32),
        jax.ShapeDtypeStruct((1, rows), f32),
        jax.ShapeDtypeStruct((D_LATENT, rows), f32),
    )
    own = pack_queries(queries, w_kv_up)
    qws = [own] + [
        lax.ppermute(own, "x", [(i, (i + k) % XS) for i in range(XS)]) for k in range(1, XS)
    ]
    shapes = (
        jax.ShapeDtypeStruct((768, rows), bf16),
        jax.ShapeDtypeStruct((2 * XS, VDIM, D_LATENT), bf16),
    )
    qcat, values = call(query_kernel, shapes, *qws)
    zs = ZH * ZL
    up = [((z, 1), ((z + 1) % zs, 1)) for z in range(zs)]
    down = [((z, 0), ((z - 1) % zs, 0)) for z in range(zs)]
    pairs = [(z * CS + c, to_z * CS + to_c) for (z, c), (to_z, to_c) in up + down]
    far = lax.ppermute(near, ("zh", "zl", "c"), pairs)
    swap = [(0, 1), (1, 0)]
    near_other = lax.ppermute(near, "c", swap)
    m, l, acc = call(attend_first, state, near, qcat)
    m, l, acc = call(functools.partial(attend_more, True, False), state, near_other, qcat, m, l, acc)
    far_other = lax.ppermute(far, "c", swap)
    m, l, acc = call(functools.partial(attend_more, False, True), state, far, qcat, m, l, acc)
    parts = call(
        attend_last,
        jax.ShapeDtypeStruct((XS, OUT_ROWS, 128), bf16),
        values, far_other, qcat, m, l, acc,
        scratch=[pltpu.VMEM(s.shape, f32) for s in state],
    )
    parts = lax.all_to_all(parts, "x", split_axis=0, concat_axis=0, tiled=True)
    return call(combine_kernel, jax.ShapeDtypeStruct((GROUP, 2 * VDIM), bf16), parts)


def solution(mesh):
    mesh = Mesh(mesh.devices.reshape(YS, ZH, ZL, CS, XS), ("y", "zh", "zl", "c", "x"))
    seq = ("y", "zh", "zl", "c")
    in_specs = (P(seq, "x"), P((*seq, "x"), None), P(None, "x"))
    return jax.shard_map(steps, mesh=mesh, in_specs=in_specs, out_specs=P(seq, "x"), check_vma=False)
```

```python
import functools
import math

import jax
import jax.numpy as jnp
from jax import lax
from jax.experimental import pallas as pl
from jax.experimental.pallas import tpu as pltpu
from jax.sharding import Mesh
from jax.sharding import PartitionSpec as P

D_LATENT = 256
ROPE = 64
NOPE = 128
VDIM = 128
MASKED = -1e30
LOWEST = -0.5e30
LOG2_SCALE = math.log2(math.e) * (NOPE + ROPE) ** -0.5


YS, ZH, ZL, CS, XS = 8, 4, 2, 2, 4
GROUP = 128
KEYS = 32
UNIT = 2 * GROUP
HALF = YS * ZH // 2
PACKED = KEYS * (D_LATENT + ROPE) // 128
VMEM_LIMIT = 20 * 2**20
OUT_ROWS = 2 * VDIM + 16
NT = (((1,), (1,)), ((), ()))
f32, bf16 = jnp.float32, jnp.bfloat16


def split(value):
    high = value.astype(bf16)
    return high, (value - high.astype(f32)).astype(bf16)


def query_kernel(*refs):
    qcat_ref, values_ref = refs[XS:]
    for k in range(XS):
        qw_ref = refs[k]
        rope = qw_ref[2 * GROUP : 3 * GROUP].astype(f32).T * LOG2_SCALE
        for h in range(2):
            nope = qw_ref[h * GROUP : (h + 1) * GROUP]
            start = 3 * GROUP + h * 2 * D_LATENT
            w_key = qw_ref[start : start + D_LATENT]
            side = lax.dot_general(w_key, nope, NT, preferred_element_type=f32) * LOG2_SCALE
            values_ref[2 * k + h] = qw_ref[start + D_LATENT : start + 2 * D_LATENT].T
            cols = pl.ds((2 * k + h) * GROUP, GROUP)
            high, low = split(side)
            qcat_ref[0:256, cols] = high
            qcat_ref[256:512, cols] = low
            high, low = split(rope[h * ROPE : (h + 1) * ROPE])
            none = jnp.zeros((ROPE, GROUP), bf16)
            qcat_ref[512:768, cols] = jnp.concatenate([high, none, low, none], axis=0)


def attend_groups(groups, kv_ref, key_zl, key_c, qcat_ref, old, new):
    y, zh, zl, c, x = (lax.axis_index(a) for a in ("y", "zh", "zl", "c", "x"))
    count, free = groups * KEYS, (groups - HALF) * KEYS
    block = kv_ref[0:groups]
    latent = jnp.concatenate(
        [block[:, 0:KEYS].reshape(count, 128), block[:, KEYS : 2 * KEYS].reshape(count, 128)], axis=1
    )
    packed = block[:, 2 * KEYS :].astype(f32)
    other = pltpu.roll(packed.reshape(count // 2, 128), 64, 1).reshape(packed.shape)
    rope = jnp.concatenate([packed, other], axis=1).astype(bf16).reshape(count, 128)
    keys = jnp.concatenate([latent, latent, rope, rope], axis=1)
    turned = latent.T
    key = free + lax.broadcasted_iota(jnp.int32, (count - free, UNIT), 0)
    row = lax.broadcasted_iota(jnp.int32, (count - free, UNIT), 1) % GROUP
    query_pos = (((y * ZH + zh) * ZL + zl) * CS + c) * GROUP + row
    key_pos = (((key // KEYS) * ZL + key_zl) * CS + key_c) * GROUP + x * KEYS + key % KEYS
    allowed = key_pos <= query_pos
    m_ref, l_ref, acc_ref = new
    units = [pl.ds(u * UNIT, UNIT) for u in range(XS)]
    scores = [jnp.dot(keys, qcat_ref[:, cols], preferred_element_type=f32) for cols in units]
    for s, cols in zip(scores, units):
        masked = jnp.where(allowed, s[free:], MASKED)
        s = jnp.concatenate([s[:free], masked], axis=0) if free else masked
        top = jnp.max(s, axis=0, keepdims=True)
        top = jnp.maximum(top, LOWEST if old is None else old[0][:, cols])
        weights = jnp.exp2(s - top)
        total = jnp.sum(weights, axis=0, keepdims=True)
        update = jnp.dot(turned, weights.astype(bf16), preferred_element_type=f32)
        if old is not None:
            factor = jnp.exp2(old[0][:, cols] - top)
            total = total + old[1][:, cols] * factor
            update = update + old[2][:, cols] * factor
        m_ref[:, cols], l_ref[:, cols], acc_ref[:, cols] = top, total, update


def attend(same_parity, same_core, kv_ref, qcat_ref, old, new):
    zl, c = lax.axis_index("zl"), lax.axis_index("c")
    key_zl = zl if same_parity else 1 - zl
    key_c = c if same_core else 1 - c
    upper = lax.axis_index("y") >= YS // 2

    @pl.when(upper)
    def _():
        attend_groups(2 * HALF, kv_ref, key_zl, key_c, qcat_ref, old, new)

    @pl.when(jnp.logical_not(upper))
    def _():
        attend_groups(HALF, kv_ref, key_zl, key_c, qcat_ref, old, new)


def attend_first(kv_ref, qcat_ref, m_ref, l_ref, acc_ref):
    attend(True, True, kv_ref, qcat_ref, None, (m_ref, l_ref, acc_ref))


def attend_more(same_parity, same_core, kv_ref, qcat_ref, m_in, l_in, acc_in, m_ref, l_ref, acc_ref):
    attend(same_parity, same_core, kv_ref, qcat_ref, (m_in, l_in, acc_in), (m_ref, l_ref, acc_ref))


def thirds(value):
    high, _ = split(value)
    middle, low = split(value - high.astype(f32))
    return [high, middle, low]


def attend_last(values_ref, kv_ref, qcat_ref, m_in, l_in, acc_in, out_ref, m_ref, l_ref, acc_ref):
    attend_more(False, False, kv_ref, qcat_ref, m_in, l_in, acc_in, m_ref, l_ref, acc_ref)
    x = lax.axis_index("x")
    for k in range(XS):
        owner = lax.rem(x + XS - k, XS)
        stats = []
        for h in range(2):
            cols = pl.ds((2 * k + h) * GROUP, GROUP)
            w_value = values_ref[2 * k + h]
            halves = jnp.concatenate(split(acc_ref[:, cols]), axis=1)
            part = jnp.dot(w_value, halves, preferred_element_type=f32)
            part = part[:, :GROUP] + part[:, GROUP:]
            out_ref[owner, h * VDIM : (h + 1) * VDIM] = part.astype(bf16)
            stats += thirds(m_ref[:, cols]) + thirds(l_ref[:, cols])
        stats.append(jnp.zeros((4, GROUP), bf16))
        out_ref[owner, 2 * VDIM :] = jnp.concatenate([t.astype(f32) for t in stats], axis=0).astype(bf16)


def combine_kernel(parts_ref, out_ref):
    stats = [parts_ref[k, 2 * VDIM :].astype(f32) for k in range(XS)]
    for h in range(2):

        def whole(k, at):
            row = 6 * h + 3 * at
            return stats[k][row : row + 1] + stats[k][row + 1 : row + 2] + stats[k][row + 2 : row + 3]

        maxima = [whole(k, 0) for k in range(XS)]
        top = jnp.maximum(jnp.maximum(maxima[0], maxima[1]), jnp.maximum(maxima[2], maxima[3]))
        factors = [jnp.exp2(m - top) for m in maxima]
        total = sum(f * whole(k, 1) for k, f in enumerate(factors))
        numerator = sum(
            parts_ref[k, h * VDIM : (h + 1) * VDIM].astype(f32) * (f / total) for k, f in enumerate(factors)
        )
        out_ref[:, h * VDIM : (h + 1) * VDIM] = numerator.T.astype(bf16)


def call(kernel, out_shape, *args, scratch=()):
    return pl.pallas_call(
        kernel,
        out_shape=out_shape,
        in_specs=[pl.BlockSpec(memory_space=pltpu.VMEM)] * len(args),
        out_specs=jax.tree.map(lambda _: pl.BlockSpec(memory_space=pltpu.VMEM), out_shape),
        scratch_shapes=list(scratch),
        compiler_params=pltpu.CompilerParams(vmem_limit_bytes=VMEM_LIMIT),
    )(*args)


def pack_kernel(latent_ref, out_ref):
    half = KEYS // 2
    rows = latent_ref[...].astype(f32)
    rope = jnp.concatenate([rows[:half, D_LATENT:], rows[half:, D_LATENT:]], axis=1)
    packed = jnp.concatenate([rows[:, :128], rows[:, 128:256], rope], axis=0).astype(bf16)
    for i in range(YS * ZH):
        out_ref[i] = packed


def pack_queries(queries, w_kv_up):
    wide = NOPE + ROPE
    return jnp.concatenate(
        [
            queries[:, :NOPE],
            queries[:, wide : wide + NOPE],
            jnp.concatenate([queries[:, NOPE:wide], queries[:, wide + NOPE :]], axis=1),
        ]
        + [w_kv_up[:, i * 128 : (i + 1) * 128] for i in range(4)],
        axis=0,
    )


def steps(queries, latent, w_kv_up):
    copies = call(pack_kernel, jax.ShapeDtypeStruct((YS * ZH, PACKED, 128), bf16), latent)
    near = lax.all_to_all(copies, ("y", "zh"), split_axis=0, concat_axis=0, tiled=True)
    rows = XS * UNIT
    state = (
        jax.ShapeDtypeStruct((1, rows), f32),
        jax.ShapeDtypeStruct((1, rows), f32),
        jax.ShapeDtypeStruct((D_LATENT, rows), f32),
    )
    own = pack_queries(queries, w_kv_up)
    qws = [own] + [
        lax.ppermute(own, "x", [(i, (i + k) % XS) for i in range(XS)]) for k in range(1, XS)
    ]
    shapes = (
        jax.ShapeDtypeStruct((768, rows), bf16),
        jax.ShapeDtypeStruct((2 * XS, VDIM, D_LATENT), bf16),
    )
    qcat, values = call(query_kernel, shapes, *qws)
    zs = ZH * ZL
    pairs = [(z * CS, (z ^ 1) * CS) for z in range(zs)]
    pairs += [(z * CS + 1, ((z + 1 if z % 2 else z - 1) % zs) * CS + 1) for z in range(zs)]
    far = lax.ppermute(near, ("zh", "zl", "c"), pairs)
    swap = [(0, 1), (1, 0)]
    near_other = lax.ppermute(near, "c", swap)
    m, l, acc = call(attend_first, state, near, qcat)
    m, l, acc = call(functools.partial(attend_more, True, False), state, near_other, qcat, m, l, acc)
    far_other = lax.ppermute(far, "c", swap)
    m, l, acc = call(functools.partial(attend_more, False, True), state, far, qcat, m, l, acc)
    parts = call(
        attend_last,
        jax.ShapeDtypeStruct((XS, OUT_ROWS, 128), bf16),
        values, far_other, qcat, m, l, acc,
        scratch=[pltpu.VMEM(s.shape, f32) for s in state],
    )
    parts = lax.all_to_all(parts, "x", split_axis=0, concat_axis=0, tiled=True)
    return call(combine_kernel, jax.ShapeDtypeStruct((GROUP, 2 * VDIM), bf16), parts)


def solution(mesh):
    mesh = Mesh(mesh.devices.reshape(YS, ZH, ZL, CS, XS), ("y", "zh", "zl", "c", "x"))
    seq = ("y", "zh", "zl", "c")
    in_specs = (P(seq, "x"), P((*seq, "x"), None), P(None, "x"))
    return jax.shard_map(steps, mesh=mesh, in_specs=in_specs, out_specs=P(seq, "x"), check_vma=False)
```

```python
import functools
import math

import jax
import jax.numpy as jnp
from jax import lax
from jax.experimental import pallas as pl
from jax.experimental.pallas import tpu as pltpu
from jax.sharding import Mesh
from jax.sharding import PartitionSpec as P

D_LATENT = 256
ROPE = 64
NOPE = 128
VDIM = 128
MASKED = -1e30
LOWEST = -0.5e30
LOG2_SCALE = math.log2(math.e) * (NOPE + ROPE) ** -0.5


YS, ZH, ZL, CS, XS = 8, 4, 2, 2, 4
GROUP = 128
KEYS = 32
UNIT = 2 * GROUP
HALF = YS * ZH // 2
PACKED = KEYS * (D_LATENT + ROPE) // 128
VMEM_LIMIT = 20 * 2**20
OUT_ROWS = 2 * VDIM + 16
NT = (((1,), (1,)), ((), ()))
f32, bf16 = jnp.float32, jnp.bfloat16


def split(value):
    high = value.astype(bf16)
    return high, (value - high.astype(f32)).astype(bf16)


def query_kernel(*refs):
    qcat_ref, values_ref = refs[XS:]
    for k in range(XS):
        qw_ref = refs[k]
        rope = qw_ref[2 * GROUP : 3 * GROUP].astype(f32).T * LOG2_SCALE
        for h in range(2):
            nope = qw_ref[h * GROUP : (h + 1) * GROUP]
            start = 3 * GROUP + h * 2 * D_LATENT
            w_key = qw_ref[start : start + D_LATENT]
            side = lax.dot_general(w_key, nope, NT, preferred_element_type=f32) * LOG2_SCALE
            values_ref[2 * k + h] = qw_ref[start + D_LATENT : start + 2 * D_LATENT].T
            cols = pl.ds((2 * k + h) * GROUP, GROUP)
            high, low = split(side)
            qcat_ref[0:256, cols] = high
            qcat_ref[256:512, cols] = low
            high, low = split(rope[h * ROPE : (h + 1) * ROPE])
            none = jnp.zeros((ROPE, GROUP), bf16)
            qcat_ref[512:768, cols] = jnp.concatenate([high, none, low, none], axis=0)


def attend_groups(groups, kv_ref, key_zl, key_c, qcat_ref, old, new):
    y, zh, zl, c, x = (lax.axis_index(a) for a in ("y", "zh", "zl", "c", "x"))
    count, free = groups * KEYS, max(groups - HALF, 0) * KEYS
    block = kv_ref[0:groups]
    latent = jnp.concatenate(
        [block[:, 0:KEYS].reshape(count, 128), block[:, KEYS : 2 * KEYS].reshape(count, 128)], axis=1
    )
    packed = block[:, 2 * KEYS :].astype(f32)
    other = pltpu.roll(packed.reshape(count // 2, 128), 64, 1).reshape(packed.shape)
    rope = jnp.concatenate([packed, other], axis=1).astype(bf16).reshape(count, 128)
    keys = jnp.concatenate([latent, latent, rope, rope], axis=1)
    turned = latent.T
    key = free + lax.broadcasted_iota(jnp.int32, (count - free, UNIT), 0)
    row = lax.broadcasted_iota(jnp.int32, (count - free, UNIT), 1) % GROUP
    query_pos = (((y * ZH + zh) * ZL + zl) * CS + c) * GROUP + row
    key_pos = (((key // KEYS) * ZL + key_zl) * CS + key_c) * GROUP + x * KEYS + key % KEYS
    allowed = key_pos <= query_pos
    m_ref, l_ref, acc_ref = new
    units = [pl.ds(u * UNIT, UNIT) for u in range(XS)]
    scores = [jnp.dot(keys, qcat_ref[:, cols], preferred_element_type=f32) for cols in units]
    for s, cols in zip(scores, units):
        masked = jnp.where(allowed, s[free:], MASKED)
        s = jnp.concatenate([s[:free], masked], axis=0) if free else masked
        top = jnp.max(s, axis=0, keepdims=True)
        top = jnp.maximum(top, LOWEST if old is None else old[0][:, cols])
        weights = jnp.exp2(s - top)
        total = jnp.sum(weights, axis=0, keepdims=True)
        update = jnp.dot(turned, weights.astype(bf16), preferred_element_type=f32)
        if old is not None:
            factor = jnp.exp2(old[0][:, cols] - top)
            total = total + old[1][:, cols] * factor
            update = update + old[2][:, cols] * factor
        m_ref[:, cols], l_ref[:, cols], acc_ref[:, cols] = top, total, update


def attend(same_parity, same_core, kv_ref, qcat_ref, old, new):
    zl, c = lax.axis_index("zl"), lax.axis_index("c")
    key_zl = zl if same_parity else 1 - zl
    key_c = c if same_core else 1 - c
    y = lax.axis_index("y")

    @pl.when(y >= YS // 2)
    def _():
        attend_groups(2 * HALF, kv_ref, key_zl, key_c, qcat_ref, old, new)

    @pl.when((y >= YS // 4) & (y < YS // 2))
    def _():
        attend_groups(HALF, kv_ref, key_zl, key_c, qcat_ref, old, new)

    @pl.when(y < YS // 4)
    def _():
        attend_groups(HALF // 2, kv_ref, key_zl, key_c, qcat_ref, old, new)


def attend_first(kv_ref, qcat_ref, m_ref, l_ref, acc_ref):
    attend(True, True, kv_ref, qcat_ref, None, (m_ref, l_ref, acc_ref))


def attend_more(same_parity, same_core, kv_ref, qcat_ref, m_in, l_in, acc_in, m_ref, l_ref, acc_ref):
    attend(same_parity, same_core, kv_ref, qcat_ref, (m_in, l_in, acc_in), (m_ref, l_ref, acc_ref))


def thirds(value):
    high, _ = split(value)
    middle, low = split(value - high.astype(f32))
    return [high, middle, low]


def attend_last(values_ref, kv_ref, qcat_ref, m_in, l_in, acc_in, out_ref, m_ref, l_ref, acc_ref):
    attend_more(False, False, kv_ref, qcat_ref, m_in, l_in, acc_in, m_ref, l_ref, acc_ref)
    x = lax.axis_index("x")
    for k in range(XS):
        owner = lax.rem(x + XS - k, XS)
        stats = []
        for h in range(2):
            cols = pl.ds((2 * k + h) * GROUP, GROUP)
            w_value = values_ref[2 * k + h]
            halves = jnp.concatenate(split(acc_ref[:, cols]), axis=1)
            part = jnp.dot(w_value, halves, preferred_element_type=f32)
            part = part[:, :GROUP] + part[:, GROUP:]
            out_ref[owner, h * VDIM : (h + 1) * VDIM] = part.astype(bf16)
            stats += thirds(m_ref[:, cols]) + thirds(l_ref[:, cols])
        stats.append(jnp.zeros((4, GROUP), bf16))
        out_ref[owner, 2 * VDIM :] = jnp.concatenate([t.astype(f32) for t in stats], axis=0).astype(bf16)


def combine_kernel(parts_ref, out_ref):
    stats = [parts_ref[k, 2 * VDIM :].astype(f32) for k in range(XS)]
    for h in range(2):

        def whole(k, at):
            row = 6 * h + 3 * at
            return stats[k][row : row + 1] + stats[k][row + 1 : row + 2] + stats[k][row + 2 : row + 3]

        maxima = [whole(k, 0) for k in range(XS)]
        top = jnp.maximum(jnp.maximum(maxima[0], maxima[1]), jnp.maximum(maxima[2], maxima[3]))
        factors = [jnp.exp2(m - top) for m in maxima]
        total = sum(f * whole(k, 1) for k, f in enumerate(factors))
        numerator = sum(
            parts_ref[k, h * VDIM : (h + 1) * VDIM].astype(f32) * (f / total) for k, f in enumerate(factors)
        )
        out_ref[:, h * VDIM : (h + 1) * VDIM] = numerator.T.astype(bf16)


def call(kernel, out_shape, *args, scratch=()):
    return pl.pallas_call(
        kernel,
        out_shape=out_shape,
        in_specs=[pl.BlockSpec(memory_space=pltpu.VMEM)] * len(args),
        out_specs=jax.tree.map(lambda _: pl.BlockSpec(memory_space=pltpu.VMEM), out_shape),
        scratch_shapes=list(scratch),
        compiler_params=pltpu.CompilerParams(vmem_limit_bytes=VMEM_LIMIT),
    )(*args)


def pack_kernel(latent_ref, out_ref):
    half = KEYS // 2
    rows = latent_ref[...].astype(f32)
    rope = jnp.concatenate([rows[:half, D_LATENT:], rows[half:, D_LATENT:]], axis=1)
    packed = jnp.concatenate([rows[:, :128], rows[:, 128:256], rope], axis=0).astype(bf16)
    for i in range(YS * ZH):
        out_ref[i] = packed


def pack_queries(queries, w_kv_up):
    wide = NOPE + ROPE
    return jnp.concatenate(
        [
            queries[:, :NOPE],
            queries[:, wide : wide + NOPE],
            jnp.concatenate([queries[:, NOPE:wide], queries[:, wide + NOPE :]], axis=1),
        ]
        + [w_kv_up[:, i * 128 : (i + 1) * 128] for i in range(4)],
        axis=0,
    )


def steps(queries, latent, w_kv_up):
    copies = call(pack_kernel, jax.ShapeDtypeStruct((YS * ZH, PACKED, 128), bf16), latent)
    near = lax.all_to_all(copies, ("y", "zh"), split_axis=0, concat_axis=0, tiled=True)
    rows = XS * UNIT
    state = (
        jax.ShapeDtypeStruct((1, rows), f32),
        jax.ShapeDtypeStruct((1, rows), f32),
        jax.ShapeDtypeStruct((D_LATENT, rows), f32),
    )
    own = pack_queries(queries, w_kv_up)
    qws = [own] + [
        lax.ppermute(own, "x", [(i, (i + k) % XS) for i in range(XS)]) for k in range(1, XS)
    ]
    shapes = (
        jax.ShapeDtypeStruct((768, rows), bf16),
        jax.ShapeDtypeStruct((2 * XS, VDIM, D_LATENT), bf16),
    )
    qcat, values = call(query_kernel, shapes, *qws)
    zs = ZH * ZL
    pairs = [(z * CS, (z ^ 1) * CS) for z in range(zs)]
    pairs += [(z * CS + 1, ((z + 1 if z % 2 else z - 1) % zs) * CS + 1) for z in range(zs)]
    far = lax.ppermute(near, ("zh", "zl", "c"), pairs)
    swap = [(0, 1), (1, 0)]
    near_other = lax.ppermute(near, "c", swap)
    m, l, acc = call(attend_first, state, near, qcat)
    m, l, acc = call(functools.partial(attend_more, True, False), state, near_other, qcat, m, l, acc)
    far_other = lax.ppermute(far, "c", swap)
    m, l, acc = call(functools.partial(attend_more, False, True), state, far, qcat, m, l, acc)
    parts = call(
        attend_last,
        jax.ShapeDtypeStruct((XS, OUT_ROWS, 128), bf16),
        values, far_other, qcat, m, l, acc,
        scratch=[pltpu.VMEM(s.shape, f32) for s in state],
    )
    parts = lax.all_to_all(parts, "x", split_axis=0, concat_axis=0, tiled=True)
    return call(combine_kernel, jax.ShapeDtypeStruct((GROUP, 2 * VDIM), bf16), parts)


def solution(mesh):
    mesh = Mesh(mesh.devices.reshape(YS, ZH, ZL, CS, XS), ("y", "zh", "zl", "c", "x"))
    seq = ("y", "zh", "zl", "c")
    in_specs = (P(seq, "x"), P((*seq, "x"), None), P(None, "x"))
    return jax.shard_map(steps, mesh=mesh, in_specs=in_specs, out_specs=P(seq, "x"), check_vma=False)
```
